16 devices in a mesh: dp: 2 (over y, z), tp: 8 (over x, core).
Axes of the slice: x: 4, y: 2, z: 1, core: 2. Of those that a mesh axis runs over, the one named last changes fastest.
The devices are a block of a 4x4x8 slice.
Arguments:
- token_ids: int32 [16384], P('dp'), parts along dimension 0
- embed_table: bfloat16 [151936, 896], P('tp')
- norm_gain: bfloat16 [896], replicated
- w_in: bfloat16 [896, 4864], P(None, 'tp')
- w_out: bfloat16 [4864, 896], P('tp')
Outputs:
- output: bfloat16 [16384, 896], P(('dp', 'tp')), parts along dimension 0
There are 2 independent parts. The reference program is written for one: setup_inputs(seed, part) draws one part's arguments, and reference() takes and returns one part's arrays. A program takes and returns all parts, laid end to end along the dimension named above; an argument that names none is the same for every part.
All inputs are finite; a program needn't handle non-finite values.
Results may differ from the reference program's by a relative error of at most 0.0079017.
Values are sent between devices in bfloat16 or wider.
A program may use at most 768 MiB of HBM per device.

```python
import math
import jax
import jax.numpy as jnp
from jax import lax

TOKENS = 8192
VOCAB_SIZE = 151936
MODEL_DIM = 896
MLP_WIDTH = 4864
RMS_EPS = 1e-6
ROW_BLOCK = math.gcd(TOKENS, 256)


def draw_token_ids(key):
    key_mix, key_low, key_all, key_first, key_last = jax.random.split(key, 5)
    choose_low = jax.random.randint(key_mix, (TOKENS,), 0, 4) == 0
    low_ids = jax.random.randint(key_low, (TOKENS,), 0, VOCAB_SIZE // 8)
    any_ids = jax.random.randint(key_all, (TOKENS,), 0, VOCAB_SIZE)
    token_ids = jnp.where(choose_low, low_ids, any_ids)
    first_pos = jax.random.randint(key_first, (), 0, TOKENS // 2)
    last_pos = jax.random.randint(key_last, (), TOKENS // 2, TOKENS)
    token_ids = token_ids.at[first_pos].set(0).at[last_pos].set(VOCAB_SIZE - 1)
    return token_ids.astype(jnp.int32)


def setup_inputs(seed: int = 0, part: int = 0) -> dict:
    base_key = jax.random.key(seed)
    key_ids = jax.random.fold_in(jax.random.fold_in(base_key, 1), part)
    key_table, key_gain, key_in, key_out = jax.random.split(jax.random.fold_in(base_key, 2), 4)
    embed_table = jax.random.normal(key_table, (VOCAB_SIZE, MODEL_DIM), jnp.float32)
    norm_gain = jax.random.uniform(key_gain, (MODEL_DIM,), jnp.float32, 0.5, 1.5)
    w_in = jax.random.normal(key_in, (MODEL_DIM, MLP_WIDTH), jnp.float32) * MODEL_DIM ** -0.5
    w_out = jax.random.normal(key_out, (MLP_WIDTH, MODEL_DIM), jnp.float32) * MLP_WIDTH ** -0.5
    return {
        "token_ids": draw_token_ids(key_ids),
        "embed_table": embed_table.astype(jnp.bfloat16),
        "norm_gain": norm_gain.astype(jnp.bfloat16),
        "w_in": w_in.astype(jnp.bfloat16),
        "w_out": w_out.astype(jnp.bfloat16),
    }


def block_forward(embed_rows, norm_gain, w_in, w_out):
    rows_f32 = embed_rows.astype(jnp.float32)
    inv_rms = lax.rsqrt(jnp.mean(rows_f32 * rows_f32, axis=-1, keepdims=True) + RMS_EPS)
    normed = (rows_f32 * inv_rms * norm_gain.astype(jnp.float32)).astype(jnp.bfloat16)
    pre_act = jnp.dot(normed, w_in, preferred_element_type=jnp.float32).astype(jnp.bfloat16)
    activated = jax.nn.gelu(pre_act.astype(jnp.float32), approximate=True).astype(jnp.bfloat16)
    mlp_sum = jnp.dot(activated, w_out, preferred_element_type=jnp.float32)
    return (rows_f32 + mlp_sum).astype(jnp.bfloat16)


def reference(token_ids, embed_table, norm_gain, w_in, w_out):
    embedded = jnp.take(embed_table, token_ids, axis=0)
    row_blocks = embedded.reshape(TOKENS // ROW_BLOCK, ROW_BLOCK, MODEL_DIM)
    outputs = lax.map(lambda row_blk: block_forward(row_blk, norm_gain, w_in, w_out), row_blocks)
    return outputs.reshape(TOKENS, MODEL_DIM)
```

```python
import functools

import jax
import jax.numpy as jnp
from jax import lax
from jax.experimental import pallas as pl
from jax.experimental.pallas import tpu as pltpu
from jax.sharding import PartitionSpec as P

RMS_EPS = 1e-6
MESH = pl.DeviceIdType.MESH
SUB = 8
GELU_C = 0.7978845608028654
MIB = 2**20


def pick_rows(rows, idx_ref, base):
    width = rows.shape[-1]
    iota = lax.broadcasted_iota(jnp.int32, (SUB, width), 0)
    acc = jnp.zeros((SUB, width), jnp.float32)
    for p in range(SUB):
        idx = idx_ref[base + p]
        row = jnp.maximum(idx, 0)
        tile = rows[lax.shift_right_logical(row, 3)].astype(jnp.float32)
        tile = pltpu.roll(tile, (p + SUB - (row & 7)) & 7, 0)
        acc = jnp.where(iota == jnp.where(idx >= 0, p, SUB), tile, acc)
    return acc


def gather_kernel(chunks, groups, idx_ref, table_hbm, out_ref, table, sem):
    step = pl.program_id(0)
    tiles = table.shape[0]

    @pl.when(step == 0)
    def _():
        copies = []
        for i in range(chunks):
            lo, hi = tiles * i // chunks, tiles * (i + 1) // chunks
            part = pl.ds(lo, hi - lo)
            copies.append(pltpu.make_async_copy(table_hbm.at[part], table.at[part], sem.at[i]))
        for copy in copies:
            copy.start()
        for copy in copies:
            copy.wait()

    def body(group, carry):
        out_ref[group] = pick_rows(table, idx_ref, (step * groups + group) * SUB).astype(jnp.bfloat16)
        return carry

    lax.fori_loop(0, groups, body, 0, unroll=2)


def gather_rows(idx, table, groups=64):
    width = table.shape[1]
    table3 = table.reshape(table.shape[0] // SUB, SUB, width)
    count = idx.shape[0] // SUB
    chunks = 8
    return pl.pallas_call(
        functools.partial(gather_kernel, chunks, groups),
        out_shape=jax.ShapeDtypeStruct((count, SUB, width), jnp.bfloat16),
        grid_spec=pltpu.PrefetchScalarGridSpec(
            num_scalar_prefetch=1,
            grid=(count // groups,),
            in_specs=[pl.BlockSpec(memory_space=pl.ANY)],
            out_specs=pl.BlockSpec((groups, SUB, width), lambda i, _: (i, 0, 0)),
            scratch_shapes=[pltpu.VMEM(table3.shape, jnp.bfloat16), pltpu.SemaphoreType.DMA((chunks,))],
        ),
        compiler_params=pltpu.CompilerParams(vmem_limit_bytes=48 * MIB),
    )(idx, table3)


def block_kernel(chips, ridx, sent_hbm, gain_ref, w1_hbm, w2_hbm, out_ref,
                 own, sib_part, got, fwd_up, fwd_dn, w1, w2, x_ref, n_ref, y_ref,
                 loc_sem, d2d_s, d2d_r, row_s, row_r, wx_s, wx_r, wy_s, wy_r, wd_s, wd_r):
    dp, tp = lax.axis_index("dp"), lax.axis_index("tp")
    chip, core = tp // 2, lax.rem(tp, 2)
    half = lax.rem(dp, 2)
    other = 1 - core
    sib = {"tp": chip * 2 + other}
    up = {"tp": lax.rem(chip + 1, chips) * 2 + core}
    dn = {"tp": lax.rem(chip + chips - 1, chips) * 2 + core}
    pair = {"dp": dp + 1 - 2 * half}
    groups = own.shape[1]
    mid = groups // 2
    k_in, width = w1.shape[1], w2.shape[1]
    r1 = pl.ds(pl.multiple_of(half * (k_in // 2), k_in // 2), k_in // 2)
    r2 = pl.ds(pl.multiple_of(half * (width // 2), width // 2), width // 2)

    def rcopy(src, dst, ss, rs, dev):
        return pltpu.make_async_remote_copy(src_ref=src, dst_ref=dst, send_sem=ss, recv_sem=rs,
                                            device_id=dev, device_id_type=MESH)

    barrier = pltpu.get_barrier_semaphore()
    for dev in (sib, up, dn, pair):
        pl.semaphore_signal(barrier, inc=1, device_id=dev, device_id_type=MESH)
    pl.semaphore_wait(barrier, 4)

    def mine(j):
        return j * 2 + core

    def theirs(j):
        return j * 2 + other

    wx = {
        (1, 1): rcopy(w1_hbm.at[r1], w1.at[mine(1), r1], wx_s.at[0], wx_r.at[0], up),
        (3, 1): rcopy(w1_hbm.at[r1], w1.at[mine(3), r1], wx_s.at[1], wx_r.at[1], dn),
        (1, 2): rcopy(w2_hbm.at[r2], w2.at[mine(1), r2], wx_s.at[2], wx_r.at[2], up),
        (3, 2): rcopy(w2_hbm.at[r2], w2.at[mine(3), r2], wx_s.at[3], wx_r.at[3], dn),
        (2, 1): rcopy(w1.at[mine(1), r1], w1.at[mine(2), r1], wx_s.at[4], wx_r.at[4], up),
        (2, 2): rcopy(w2.at[mine(3), r2], w2.at[mine(2), r2], wx_s.at[5], wx_r.at[5], dn),
    }
    wy, wd = {}, {}
    for j in (1, 2, 3):
        wy[j, 1] = rcopy(w1.at[mine(j), r1], w1.at[mine(j), r1], wy_s.at[2 * j - 2], wy_r.at[2 * j - 2], pair)
        wy[j, 2] = rcopy(w2.at[mine(j), r2], w2.at[mine(j), r2], wy_s.at[2 * j - 1], wy_r.at[2 * j - 1], pair)
    for j in (0, 1, 2, 3):
        s1, s2 = (w1_hbm, w2_hbm) if j == 0 else (w1.at[mine(j)], w2.at[mine(j)])
        wd[j, 1] = rcopy(s1, w1.at[mine(j)], wd_s.at[2 * j], wd_r.at[2 * j], sib)
        wd[j, 2] = rcopy(s2, w2.at[mine(j)], wd_s.at[2 * j + 1], wd_r.at[2 * j + 1], sib)

    d2d, loc = {}, {}
    for j in range(4):
        dest = lax.rem(chip + j, chips) * 2
        d2d[j] = rcopy(sent_hbm.at[dest + other], sib_part.at[j], d2d_s.at[j], d2d_r.at[j], sib)
        loc[j] = pltpu.make_async_copy(sent_hbm.at[dest + core], own.at[j], loc_sem.at[j])
    w1_loc = pltpu.make_async_copy(w1_hbm, w1.at[mine(0)], loc_sem.at[4])
    w2_loc = pltpu.make_async_copy(w2_hbm, w2.at[mine(0)], loc_sem.at[5])

    lo, hi = pl.ds(0, mid), pl.ds(mid, groups - mid)

    def slot(j, part=None):
        if part is None:
            return got.at[pl.ds(j * groups, groups)]
        return got.at[pl.ds(j * groups + part * mid, mid)]

    rows = {
        "2u": rcopy(own.at[2, lo], fwd_up, row_s.at[0], row_r.at[0], up),
        "2d": rcopy(own.at[2, hi], fwd_dn, row_s.at[1], row_r.at[1], dn),
        "1": rcopy(own.at[1], slot(1), row_s.at[2], row_r.at[2], up),
        "3": rcopy(own.at[3], slot(3), row_s.at[3], row_r.at[3], dn),
        "fu": rcopy(fwd_up, slot(2, 0), row_s.at[4], row_r.at[4], up),
        "fd": rcopy(fwd_dn, slot(2, 1), row_s.at[5], row_r.at[5], dn),
    }

    for key in ((1, 1), (3, 1), (1, 2), (3, 2)):
        wx[key].start()
    for j in (2, 1, 3, 0):
        d2d[j].start()
        loc[j].start()
    wd[0, 1].start()
    wd[0, 2].start()
    w1_loc.start()
    w2_loc.start()

    batch = 4
    for j in (2, 1, 3, 0):
        d2d[j].wait_recv()
        loc[j].wait()

        def add(i, carry, j=j):
            part = pl.ds(i * batch, batch)
            total = own[j, part] + sib_part[j, part]
            if j == 0:
                got[part] = total
            else:
                own[j, part] = total
            return carry

        lax.fori_loop(0, groups // batch, add, 0)
        if j == 2:
            rows["2u"].start()
            rows["2d"].start()
        elif j:
            rows[str(j)].start()

    wx[1, 1].wait_recv()
    wx[2, 1].start()
    wy[1, 1].start()
    wx[3, 1].wait_recv()
    wy[3, 1].start()
    wx[3, 2].wait_recv()
    wx[2, 2].start()
    wy[3, 2].start()
    wx[1, 2].wait_recv()
    wy[1, 2].start()
    rows["2u"].wait_recv()
    rows["fu"].start()
    rows["2d"].wait_recv()
    rows["fd"].start()
    for j, m in ((1, 1), (3, 1), (3, 2), (1, 2)):
        wy[j, m].wait_recv()
        wd[j, m].start()
    wx[2, 1].wait_recv()
    wy[2, 1].start()
    wx[2, 2].wait_recv()
    wy[2, 2].start()
    for key in ("1", "3", "fu", "fd"):
        rows[key].wait_recv()

    gain = gain_ref[...].astype(jnp.float32)

    def take(i, carry):
        x = jnp.concatenate([pick_rows(got, ridx, i * 16), pick_rows(got, ridx, i * 16 + SUB)], axis=0)
        inv = lax.rsqrt(jnp.mean(x * x, axis=-1, keepdims=True) + RMS_EPS)
        at = pl.ds(pl.multiple_of(i * 16, 16), 16)
        x_ref[at, :] = x.astype(jnp.bfloat16)
        n_ref[at, :] = (x * inv * gain).astype(jnp.bfloat16)
        return carry

    tokens = out_ref.shape[0]
    lax.fori_loop(0, tokens // 16, take, 0)

    block = 256

    def mlp(s, first=False, last=False):
        def body(i, carry):
            at = pl.ds(pl.multiple_of(i * block, block), block)
            u = jnp.dot(n_ref[at, :], w1[s], preferred_element_type=jnp.float32)
            z = u.astype(jnp.bfloat16).astype(jnp.float32)
            h = 0.5 * z * (1.0 + jnp.tanh(GELU_C * (z + 0.044715 * (z * z * z))))
            y = jnp.dot(h.astype(jnp.bfloat16), w2[s], preferred_element_type=jnp.float32)
            if not first:
                y = y_ref[at, :] + y
            if last:
                out_ref[at, :] = (x_ref[at, :].astype(jnp.float32) + y).astype(jnp.bfloat16)
            else:
                y_ref[at, :] = y
            return carry

        lax.fori_loop(0, tokens // block, body, 0)

    w1_loc.wait()
    w2_loc.wait()
    mlp(mine(0), first=True)
    wd[0, 1].wait_recv()
    wd[0, 2].wait_recv()
    mlp(theirs(0))
    for m in (1, 2):
        wy[2, m].wait_recv()
        wd[2, m].start()
    for j in (1, 3, 2):
        mlp(mine(j))
        wd[j, 1].wait_recv()
        wd[j, 2].wait_recv()
        mlp(theirs(j), last=j == 2)

    for table in (wx, wy, wd, d2d, rows):
        for copy in table.values():
            copy.wait_send()


def solution(mesh):
    chips = mesh.shape["tp"] // 2

    def device_step(token_ids, table, norm_gain, w1, w2):
        shard_rows, width = table.shape
        ranks = mesh.shape["tp"]
        tokens = token_ids.shape[0] // ranks
        tp = lax.axis_index("tp")
        cap = tokens
        local = token_ids - tp * shard_rows
        send_idx = jnp.where((local >= 0) & (local < shard_rows), local, -1)
        ids_mine = lax.dynamic_slice(token_ids, (tp * tokens,), (tokens,))
        rel = (tp // 2 - ids_mine // (2 * shard_rows) + chips) % chips
        ridx = rel * cap + jnp.arange(tokens, dtype=jnp.int32)
        sent = gather_rows(send_idx, table).reshape(ranks, cap // SUB, SUB, width)
        groups = cap // SUB
        hidden = w1.shape[1]
        bf, f32 = jnp.bfloat16, jnp.float32
        dma = pltpu.SemaphoreType.DMA
        anyspec = pl.BlockSpec(memory_space=pl.ANY)
        return pl.pallas_call(
            functools.partial(block_kernel, chips),
            out_shape=jax.ShapeDtypeStruct((tokens, width), bf),
            in_specs=[
                pl.BlockSpec(memory_space=pltpu.SMEM),
                anyspec,
                pl.BlockSpec(memory_space=pltpu.VMEM),
                anyspec,
                anyspec,
            ],
            out_specs=pl.BlockSpec(memory_space=pltpu.VMEM),
            scratch_shapes=[
                pltpu.VMEM((4, groups, SUB, width), bf),
                pltpu.VMEM((4, groups, SUB, width), bf),
                pltpu.VMEM((4 * groups, SUB, width), bf),
                pltpu.VMEM((groups // 2, SUB, width), bf),
                pltpu.VMEM((groups // 2, SUB, width), bf),
                pltpu.VMEM((ranks, width, hidden), bf),
                pltpu.VMEM((ranks, hidden, width), bf),
                pltpu.VMEM((tokens, width), bf),
                pltpu.VMEM((tokens, width), bf),
                pltpu.VMEM((tokens, width), f32),
                dma((6,)),
                dma((4,)), dma((4,)),
                dma((6,)), dma((6,)),
                dma((6,)), dma((6,)),
                dma((6,)), dma((6,)),
                dma((8,)), dma((8,)),
            ],
            compiler_params=pltpu.CompilerParams(
                collective_id=0, has_side_effects=True, vmem_limit_bytes=67043328
            ),
        )(ridx, sent, norm_gain.reshape(1, width), w1, w2)

    return jax.shard_map(
        device_step,
        mesh=mesh,
        in_specs=(P("dp"), P("tp", None), P(), P(None, "tp"), P("tp", None)),
        out_specs=P(("dp", "tp"), None),
        check_vma=False,
    )
```

```python
import functools

import jax
import jax.numpy as jnp
from jax import lax
from jax.experimental import pallas as pl
from jax.experimental.pallas import tpu as pltpu
from jax.sharding import PartitionSpec as P

RMS_EPS = 1e-6
MESH = pl.DeviceIdType.MESH
SUB = 8
GELU_C = 0.7978845608028654
N_COPIES = 40


def gelu(u):
    z = u.astype(jnp.bfloat16).astype(jnp.float32)
    h = 0.5 * z * (1.0 + jnp.tanh(GELU_C * (z + 0.044715 * (z * z * z))))
    return h.astype(jnp.bfloat16)


def pick_rows(rows, idx_ref, base):
    width = rows.shape[-1]
    iota = lax.broadcasted_iota(jnp.int32, (SUB, width), 0)
    acc = None
    for p in range(SUB):
        code = idx_ref[base + p]
        at = jnp.minimum(jnp.maximum(lax.shift_right_logical(code, 3), 0), rows.shape[0] - 1)
        tile = rows[at].astype(jnp.float32)
        tile = pltpu.roll(tile, (code + p) & 7, 0)
        acc = tile if acc is None else jnp.where(iota == p, tile, acc)
    return acc


def pick_16(rows, idx_ref, base):
    parts = [pick_rows(rows, idx_ref, base), pick_rows(rows, idx_ref, base + SUB)]
    return jnp.concatenate(parts, axis=0).astype(jnp.bfloat16)


def slot_tables(ids_ref, keys, slots_v, over_ref, chip, tp, chips, shard_rows, cap):
    f32 = jnp.float32
    lines = ids_ref.shape[0]
    dests = 2 * chips
    per = lines // dests
    ids = ids_ref[...]
    span = 2 * shard_rows
    lane = lax.broadcasted_iota(jnp.int32, (lines, 128), 1)
    row = lax.broadcasted_iota(jnp.int32, (lines, 128), 0) & (per - 1)
    top = None
    for s in range(chips):
        mask = (ids >= s * span) & (ids < (s + 1) * span)
        upto = jnp.where(mask, 1, 0)
        for k in range(7):
            upto = upto + jnp.where(lane >= 2**k, pltpu.roll(upto, 2**k, 1), 0)
        sums = jnp.where(lane == 127, upto, 0)
        for k in range(7):
            sums = sums + pltpu.roll(sums, 2**k, 1)
        before = jnp.where(row >= 1, pltpu.roll(sums, 1, 0), 0)
        for k in range(per.bit_length() - 1):
            before = before + jnp.where(row >= 2**k, pltpu.roll(before, 2**k, 0), 0)
        key = jnp.where(mask, upto + before - 1, -1)
        keys[pl.ds(s * lines, lines), :] = key
        key = key.astype(f32)
        top = key if top is None else jnp.maximum(top, key)
    over_ref[...] = jnp.zeros(over_ref.shape, f32) + jnp.max(top, axis=(0, 1), keepdims=True)

    lanes = slots_v.shape[1]
    slot_id = lax.broadcasted_iota(jnp.int32, (128, lanes), 1)
    first = tp * shard_rows
    none = shard_rows

    def one_dest(d, carry):
        at = pl.ds(pl.multiple_of(d * per, per), per)
        local = ids_ref[at, :] - first
        here = (local >= 0) & (local < shard_rows)
        k = keys[pl.ds(pl.multiple_of(chip * lines + d * per, per), per), :]
        key_t = jnp.transpose(jnp.where(here, k, -1))
        code = (local - (local & 7)) + ((SUB - (local & 7)) & 7)
        row_t = jnp.transpose(code - none)
        acc = jnp.zeros((128, lanes), jnp.int32)
        for r in range(per):
            acc = acc + jnp.where(key_t[:, r : r + 1] == slot_id, row_t[:, r : r + 1], 0)
        slots_v[pl.ds(d, 1), :] = jnp.clip(jnp.sum(acc, axis=0, keepdims=True) + none, 0, none)
        return carry

    lax.fori_loop(0, dests, one_dest, 0)


def block_kernel(chips, ids_ref, table_hbm, gain_ref, w1_hbm, w2_hbm, out_hbm, over_ref, w1_all, w2_all,
                 table, own, sib_part, for_sib, got, fwd_up, fwd_dn, y_ref, w_buf, keys, slots_v, sidx,
                 tab_sem, loc_sem, ss, rs):
    dp, tp = lax.axis_index("dp"), lax.axis_index("tp")
    chip, core = tp // 2, lax.rem(tp, 2)
    half = lax.rem(dp, 2)
    other = 1 - core
    sib = {"tp": chip * 2 + other}
    up = {"tp": lax.rem(chip + 1, chips) * 2 + core}
    dn = {"tp": lax.rem(chip + chips - 1, chips) * 2 + core}
    pair = {"dp": dp + 1 - 2 * half}
    cap = own.shape[0] // 3
    mid = cap // 2
    hid, width = w1_hbm.shape
    tokens = out_hbm.shape[0]
    counter = iter(range(N_COPIES))

    def rcopy(src, dst, dev):
        n = next(counter)
        return pltpu.make_async_remote_copy(src_ref=src, dst_ref=dst, send_sem=ss.at[n], recv_sem=rs.at[n],
                                            device_id=dev, device_id_type=MESH)

    n_tab = tab_sem.shape[0]
    tab_copies = []
    tiles = table.shape[0] - 1
    for i in range(n_tab):
        lo, hi = tiles * i // n_tab, tiles * (i + 1) // n_tab
        tab_copies.append(pltpu.make_async_copy(table_hbm.at[pl.ds(lo, hi - lo)], table.at[pl.ds(lo, hi - lo)],
                                                tab_sem.at[i]))

    barrier = pltpu.get_barrier_semaphore()
    for dev in (sib, up, dn, pair):
        pl.semaphore_signal(barrier, inc=1, device_id=dev, device_id_type=MESH)
    for copy in tab_copies:
        copy.start()
    pl.semaphore_wait(barrier, 4)

    hh = hid // 2

    def wrow(j, c, h=None):
        start = (j * 2 + c) * hid
        if h is None:
            return pl.ds(pl.multiple_of(start, 16), hid)
        return pl.ds(pl.multiple_of(start + h * hh, 16), hh)

    hrow = pl.ds(pl.multiple_of(half * hh, 16), hh)
    w_in = {1: w1_hbm, 2: w2_hbm}
    w_all = {1: w1_all, 2: w2_all}

    wx, wy, wd = {}, {}, {}
    for m in (1, 2):
        wx[1, m] = rcopy(w_in[m].at[hrow], w_all[m].at[wrow(1, core, half)], up)
        wx[3, m] = rcopy(w_in[m].at[hrow], w_all[m].at[wrow(3, core, half)], dn)
    split = hid * 9 // 38 // 16 * 16
    common = hid - 2 * split

    def far(j, part):
        if part == 0:
            return pl.ds(pl.multiple_of((j * 2 + core) * hid, 16), common)
        which = half if part == 1 else 1 - half
        return pl.ds(pl.multiple_of((j * 2 + core) * hid + common + which * split, 16), split)

    for part in (1, 0):
        wx[2, 1, part] = rcopy(w1_all.at[far(1, part)], w1_all.at[far(2, part)], up)
        wx[2, 2, part] = rcopy(w2_all.at[far(3, part)], w2_all.at[far(2, part)], dn)
    for m in (1, 2):
        wy[2, m] = rcopy(w_all[m].at[far(2, 1)], w_all[m].at[far(2, 1)], pair)
        for part in (0, 1, 2):
            wd[2, m, part] = rcopy(w_all[m].at[far(2, part)], w_all[m].at[far(2, part)], sib)
    for m in (1, 2):
        for j in (1, 3):
            wy[j, m] = rcopy(w_all[m].at[wrow(j, core, half)], w_all[m].at[wrow(j, core, half)], pair)
        wd[0, m] = rcopy(w_in[m], w_all[m].at[wrow(0, core)], sib)
        for j in (1, 3):
            for k, h in ((0, half), (1, 1 - half)):
                wd[j, m, k] = rcopy(w_all[m].at[wrow(j, core, h)], w_all[m].at[wrow(j, core, h)], sib)

    d2d = {}
    for n, j in enumerate((2, 1, 3, 0)):
        d2d[j] = rcopy(for_sib.at[pl.ds((n % 2) * cap, cap)], sib_part.at[pl.ds(j * cap, cap)], sib)
    rows = {
        "2u": rcopy(own.at[pl.ds(cap, mid)], fwd_up, up),
        "2d": rcopy(own.at[pl.ds(cap + mid, mid)], fwd_dn, dn),
        1: rcopy(own.at[pl.ds(0, cap)], got.at[pl.ds(cap, cap)], up),
        3: rcopy(own.at[pl.ds(2 * cap, cap)], got.at[pl.ds(3 * cap, cap)], dn),
        "fu": rcopy(fwd_up, got.at[pl.ds(2 * cap, mid)], up),
        "fd": rcopy(fwd_dn, got.at[pl.ds(2 * cap + mid, mid)], dn),
    }

    for key in ((1, 1), (3, 1), (1, 2), (3, 2)):
        wx[key].start()
    wd[0, 1].start()
    wd[0, 2].start()
    slot_tables(ids_ref, keys, slots_v, over_ref, chip, tp, chips, tiles * SUB, cap)
    table[tiles] = jnp.zeros((SUB, width), jnp.bfloat16)
    lanes = slots_v.shape[1]
    fetch = [
        pltpu.make_async_copy(slots_v.at[d], sidx.at[pl.ds(d * lanes, lanes)], loc_sem.at[4 * chips + 2 + d])
        for d in range(2 * chips)
    ]
    for copy in fetch:
        copy.start()
    for copy in fetch:
        copy.wait()
    for copy in tab_copies:
        copy.wait()

    def pick_slots(j, c, dst, at):
        base = (lax.rem(chip + j, chips) * 2 + c) * lanes

        def body(i, carry):
            dst[pl.ds(pl.multiple_of(at + i * 16, 16), 16), :] = pick_16(table, sidx, base + i * 16)
            return carry

        lax.fori_loop(0, cap // 16, body, 0)

    def add_part(j):
        d2d[j].wait_recv()
        ref, at = (got, 0) if j == 0 else (own, (j - 1) * cap)

        def body(i, carry):
            a = pl.ds(pl.multiple_of(at + i * 32, 32), 32)
            ref[a, :] = ref[a, :] + sib_part[pl.ds(pl.multiple_of(j * cap + i * 32, 32), 32), :]
            return carry

        lax.fori_loop(0, cap // 32, body, 0)

    def pick_sib(n, j):
        pick_slots(j, other, for_sib, (n % 2) * cap)
        d2d[j].start()

    def pick_own(j):
        if j == 0:
            pick_slots(j, core, got, 0)
        else:
            pick_slots(j, core, own, (j - 1) * cap)

    pick_sib(0, 2)
    pick_own(2)
    pick_sib(1, 1)
    add_part(2)
    rows["2u"].start()
    rows["2d"].start()
    pick_own(1)
    d2d[2].wait_send()
    pick_sib(2, 3)
    add_part(1)
    rows[1].start()
    for j in (1, 3):
        wx[j, 1].wait_recv()
        wy[j, 1].start()
    pick_own(3)
    add_part(3)
    rows[3].start()
    for j in (1, 3):
        wx[j, 2].wait_recv()
        wy[j, 2].start()
    d2d[1].wait_send()
    pick_sib(3, 0)
    pick_own(0)
    add_part(0)

    slot = {0: 0, 1: 1, 3: 0, 2: 1}
    piece = 2 * hid
    load = {}
    for j in range(chips):
        for m in (1, 2):
            base = (slot[j] * 2 + m - 1) * piece
            n = (j * 2 + m - 1) * 2
            if j == 0:
                load[j, m] = [
                    pltpu.make_async_copy(w_in[m], w_buf.at[pl.ds(pl.multiple_of(base + core * hid, 16), hid)],
                                          loc_sem.at[n]),
                    pltpu.make_async_copy(w_all[m].at[wrow(0, other)],
                                          w_buf.at[pl.ds(pl.multiple_of(base + other * hid, 16), hid)],
                                          loc_sem.at[n + 1]),
                ]
            else:
                load[j, m] = [
                    pltpu.make_async_copy(w_all[m].at[pl.ds(j * piece, piece)], w_buf.at[pl.ds(base, piece)],
                                          loc_sem.at[n])
                ]

    def start_load(j):
        for m in (1, 2):
            for copy in load[j, m]:
                copy.start()

    for m in (1, 2):
        wd[0, m].wait_recv()
    start_load(0)
    rows["2u"].wait_recv()
    rows["fu"].start()
    rows["2d"].wait_recv()
    rows["fd"].start()
    for j in (1, 3):
        for m in (1, 2):
            wd[j, m, 0].start()
    for m in (1, 2):
        for j in (1, 3):
            wy[j, m].wait_recv()
            wd[j, m, 1].start()
            if (j, m) == (1, 1) or (j, m) == (3, 2):
                wx[2, m, 1].start()
                wx[2, m, 0].start()

    gain = gain_ref[...].astype(jnp.float32)
    lines = tokens // 128
    slot_id = lax.broadcasted_iota(jnp.int32, (128, cap), 1).astype(jnp.float32)

    def place(sources, start, finish):
        def body(i, carry):
            at = pl.ds(pl.multiple_of(i * 512, 512), 512)
            total = None if start else y_ref[at, :]
            for j in sources:
                line = lax.rem(chip + chips - j, chips) * ids_ref.shape[0] + tp * lines
                key_t = jnp.transpose(keys[pl.ds(pl.multiple_of(line, SUB), SUB), :].astype(jnp.float32))
                lane = lax.broadcasted_iota(jnp.int32, key_t.shape, 1)
                hits = []
                for r in range(4):
                    col = jnp.sum(jnp.where(lane == 4 * i + r, key_t, 0.0), axis=1, keepdims=True)
                    hits.append(jnp.where(col == slot_id, 1.0, 0.0).astype(jnp.bfloat16))
                part = jnp.dot(jnp.concatenate(hits, axis=0), got[pl.ds(j * cap, cap), :],
                               preferred_element_type=jnp.float32)
                total = part if total is None else total + part
            if not finish:
                y_ref[at, :] = total
                return carry
            inv = lax.rsqrt(jnp.mean(total * total, axis=-1, keepdims=True) + RMS_EPS)
            sib_part[at, :] = total.astype(jnp.bfloat16)
            sib_part[pl.ds(pl.multiple_of(tokens + i * 512, 512), 512), :] = (total * inv * gain).astype(jnp.bfloat16)
            return carry

        lax.fori_loop(0, tokens // 512, body, 0)

    place((0,), True, False)
    rows[1].wait_recv()
    rows[3].wait_recv()
    place((1, 3), False, False)
    rows["fu"].wait_recv()
    rows["fd"].wait_recv()
    place((2,), False, True)

    block = 512

    def mlp(j, first=False, last=False):
        for m in (1, 2):
            for copy in load[j, m]:
                copy.wait()
        base = slot[j] * 2 * piece

        def body(i, carry):
            at = pl.ds(pl.multiple_of(i * block, block), block)
            n = sib_part[pl.ds(pl.multiple_of(tokens + i * block, block), block), :]
            u = lax.dot_general(n, w_buf[pl.ds(base, piece), :], (((1,), (1,)), ((), ())),
                                preferred_element_type=jnp.float32)
            y = jnp.dot(gelu(u), w_buf[pl.ds(base + piece, piece), :], preferred_element_type=jnp.float32)
            if not first:
                y = y_ref[at, :] + y
            if last:
                sib_part[at, :] = (sib_part[at, :].astype(jnp.float32) + y).astype(jnp.bfloat16)
            else:
                y_ref[at, :] = y
            return carry

        lax.fori_loop(0, tokens // block, body, 0)

    def arrived(j):
        for m in (1, 2):
            for k in (0, 1, 2) if j == 2 else (0, 1):
                wd[j, m, k].wait_recv()
        start_load(j)

    arrived(1)
    mlp(0, first=True)
    arrived(3)
    mlp(1)
    for m in (1, 2):
        wx[2, m, 1].wait_recv()
        wy[2, m].start()
        wd[2, m, 1].start()
    mlp(3)
    for m in (1, 2):
        wx[2, m, 0].wait_recv()
        wd[2, m, 0].start()
    for m in (1, 2):
        wy[2, m].wait_recv()
        wd[2, m, 2].start()
    arrived(2)
    mlp(2, last=True)
    store = pltpu.make_async_copy(sib_part.at[pl.ds(0, tokens)], out_hbm, loc_sem.at[4 * chips + 1])
    store.start()
    store.wait()

    d2d[3].wait_send()
    d2d[0].wait_send()
    for group in (wx, wy, wd, rows):
        for copy in group.values():
            copy.wait_send()


def copy_kernel(src, dst):
    dst[...] = src[...]


def settle(res):
    rows, width = res.shape
    spec = pl.BlockSpec((rows // 4, width), lambda i: (i, 0))
    return pl.pallas_call(
        copy_kernel,
        out_shape=jax.ShapeDtypeStruct(res.shape, res.dtype),
        grid=(4,),
        in_specs=[spec],
        out_specs=spec,
    )(res)


def solution(mesh):
    ranks = mesh.shape["tp"]
    chips = ranks // 2

    def device_step(token_ids, table, norm_gain, w1, w2):
        shard_rows, width = table.shape
        tokens = token_ids.shape[0] // ranks
        tp = lax.axis_index("tp")
        cap = tokens * 17 // 32
        hidden = w1.shape[1]
        bf, f32 = jnp.bfloat16, jnp.float32
        dma = pltpu.SemaphoreType.DMA
        anyspec = pl.BlockSpec(memory_space=pl.ANY)
        vmem = pl.BlockSpec(memory_space=pltpu.VMEM)
        lines = token_ids.shape[0] // 128
        lanes = -(-cap // 128) * 128
        out, top, w1_all, w2_all = pl.pallas_call(
            functools.partial(block_kernel, chips),
            out_shape=[
                jax.ShapeDtypeStruct((tokens, width), bf),
                jax.ShapeDtypeStruct((SUB, 128), f32),
                jax.ShapeDtypeStruct((ranks * hidden, width), bf),
                jax.ShapeDtypeStruct((ranks * hidden, width), bf),
            ],
            in_specs=[vmem, anyspec, vmem, anyspec, anyspec],
            out_specs=[anyspec, vmem, anyspec, anyspec],
            scratch_shapes=[
                pltpu.VMEM((shard_rows // SUB + 1, SUB, width), bf),
                pltpu.VMEM((3 * cap, width), bf),
                pltpu.VMEM((4 * cap, width), bf),
                pltpu.VMEM((2 * cap, width), bf),
                pltpu.VMEM((4 * cap, width), bf),
                pltpu.VMEM((cap // 2, width), bf),
                pltpu.VMEM((cap // 2, width), bf),
                pltpu.VMEM((tokens, width), f32),
                pltpu.VMEM((8 * hidden, width), bf),
                pltpu.VMEM((chips * lines, 128), jnp.int32),
                pltpu.VMEM((ranks, lanes), jnp.int32),
                pltpu.SMEM((ranks * lanes,), jnp.int32),
                dma((8,)), dma((4 * chips + 2 + ranks,)),
                dma((N_COPIES,)), dma((N_COPIES,)),
            ],
            compiler_params=pltpu.CompilerParams(
                collective_id=0, has_side_effects=True, vmem_limit_bytes=67043328
            ),
        )(token_ids.reshape(lines, 128), table.reshape(shard_rows // SUB, SUB, width), norm_gain.reshape(1, width), w1.T, w2)
        overflow = top[0, 0] >= cap

        def plain(_):
            local = token_ids - tp * shard_rows
            owned = (local >= 0) & (local < shard_rows)
            found = jnp.take(table, jnp.clip(local, 0, shard_rows - 1), axis=0, mode="clip")
            part = jnp.where(owned[:, None], found, jnp.zeros((), bf)).reshape(ranks, tokens, width)
            x = jnp.sum(lax.all_to_all(part, "tp", 0, 0).astype(f32), axis=0)
            w1s = lax.dynamic_update_slice(w1_all, w1.T, ((tp % 2) * hidden, 0))
            w2s = lax.dynamic_update_slice(w2_all, w2, ((tp % 2) * hidden, 0))
            inv = lax.rsqrt(jnp.mean(x * x, axis=-1, keepdims=True) + RMS_EPS)
            n = (x * inv * norm_gain.astype(f32)).astype(bf)
            u = lax.dot_general(n, w1s, (((1,), (1,)), ((), ())), preferred_element_type=f32)
            y = jnp.dot(gelu(u), w2s, preferred_element_type=f32)
            return (x + y).astype(bf)

        return lax.cond(overflow, plain, settle, out)

    return jax.shard_map(
        device_step,
        mesh=mesh,
        in_specs=(P("dp"), P("tp", None), P(), P(None, "tp"), P("tp", None)),
        out_specs=P(("dp", "tp"), None),
        check_vma=False,
    )
```

```python
import functools

import jax
import jax.numpy as jnp
from jax import lax
from jax.experimental import pallas as pl
from jax.experimental.pallas import tpu as pltpu
from jax.sharding import PartitionSpec as P

RMS_EPS = 1e-6
MESH = pl.DeviceIdType.MESH
SUB = 8
GELU_C = 0.7978845608028654
N_COPIES = 52


def gelu(u):
    z = u.astype(jnp.bfloat16).astype(jnp.float32)
    h = 0.5 * z * (1.0 + jnp.tanh(GELU_C * (z + 0.044715 * (z * z * z))))
    return h.astype(jnp.bfloat16)


def pick_rows(rows, idx_ref, base):
    width = rows.shape[-1]
    iota = lax.broadcasted_iota(jnp.int32, (SUB, width), 0)
    acc = None
    for p in range(SUB):
        code = idx_ref[base + p]
        at = jnp.minimum(jnp.maximum(lax.shift_right_logical(code, 3), 0), rows.shape[0] - 1)
        tile = rows[at].astype(jnp.float32)
        tile = pltpu.roll(tile, (code + p) & 7, 0)
        acc = tile if acc is None else jnp.where(iota == p, tile, acc)
    return acc


def pick_16(rows, idx_ref, base):
    parts = [pick_rows(rows, idx_ref, base), pick_rows(rows, idx_ref, base + SUB)]
    return jnp.concatenate(parts, axis=0).astype(jnp.bfloat16)


def slot_split(tokens):
    return tokens * 15 // 64, tokens * 9 // 32


def slot_tables(ids_ref, keys, slots_v, over_ref, chip, tp, chips, shard_rows, base):
    f32 = jnp.float32
    lines = ids_ref.shape[0]
    dests = 2 * chips
    per = lines // dests
    ids = ids_ref[...]
    span = 2 * shard_rows
    lane = lax.broadcasted_iota(jnp.int32, (lines, 128), 1)
    row = lax.broadcasted_iota(jnp.int32, (lines, 128), 0) & (per - 1)

    def scan(mask):
        upto = jnp.where(mask, 1, 0)
        for k in range(7):
            upto = upto + jnp.where(lane >= 2**k, pltpu.roll(upto, 2**k, 1), 0)
        sums = jnp.where(lane == 127, upto, 0)
        for k in range(7):
            sums = sums + pltpu.roll(sums, 2**k, 1)
        before = jnp.where(row >= 1, pltpu.roll(sums, 1, 0), 0)
        for k in range(per.bit_length() - 1):
            before = before + jnp.where(row >= 2**k, pltpu.roll(before, 2**k, 0), 0)
        return upto + before - 1

    ranks = []
    extra = None
    for s in range(chips):
        mask = (ids >= s * span) & (ids < (s + 1) * span)
        rank = jnp.where(mask, scan(mask), -1)
        ranks.append(rank)
        extra = rank if extra is None else jnp.maximum(extra, rank)
    shared = scan(extra >= base) + base
    top = None
    for s in range(chips):
        key = jnp.where(ranks[s] >= base, shared, ranks[s])
        keys[pl.ds(s * lines, lines), :] = key
        key = key.astype(f32)
        top = key if top is None else jnp.maximum(top, key)
    over_ref[...] = jnp.zeros(over_ref.shape, f32) + jnp.max(top, axis=(0, 1), keepdims=True)

    lanes = slots_v.shape[1]
    slot_id = lax.broadcasted_iota(jnp.int32, (128, lanes), 1)
    first = tp * shard_rows
    none = shard_rows

    def one_dest(d, carry):
        at = pl.ds(pl.multiple_of(d * per, per), per)
        local = ids_ref[at, :] - first
        here = (local >= 0) & (local < shard_rows)
        k = keys[pl.ds(pl.multiple_of(chip * lines + d * per, per), per), :]
        key_t = jnp.transpose(jnp.where(here, k, -1))
        code = (local - (local & 7)) + ((SUB - (local & 7)) & 7)
        row_t = jnp.transpose(code - none)
        acc = jnp.zeros((128, lanes), jnp.int32)
        for r in range(per):
            acc = acc + jnp.where(key_t[:, r : r + 1] == slot_id, row_t[:, r : r + 1], 0)
        slots_v[pl.ds(d, 1), :] = jnp.clip(jnp.sum(acc, axis=0, keepdims=True) + none, 0, none)
        return carry

    lax.fori_loop(0, dests, one_dest, 0)


def block_kernel(chips, ids_ref, table_hbm, gain_ref, w1_hbm, w2_hbm, out_hbm, over_ref, w1_all, w2_all,
                 table, own, sib_part, for_sib, got, fwd_up, fwd_dn, y_ref, w_buf, keys, slots_v, sidx,
                 tab_sem, loc_sem, ss, rs):
    dp, tp = lax.axis_index("dp"), lax.axis_index("tp")
    chip, core = tp // 2, lax.rem(tp, 2)
    half = lax.rem(dp, 2)
    other = 1 - core
    sib = {"tp": chip * 2 + other}
    up = {"tp": lax.rem(chip + 1, chips) * 2 + core}
    dn = {"tp": lax.rem(chip + chips - 1, chips) * 2 + core}
    pair = {"dp": dp + 1 - 2 * half}
    cap = own.shape[0] // 3
    hid, width = w1_hbm.shape
    tokens = out_hbm.shape[0]
    base, ext = slot_split(tokens)
    eh = ext // 2
    b_lo = fwd_up.shape[0] - eh
    b_hi = base - b_lo
    counter = iter(range(N_COPIES))

    def rcopy(src, dst, dev):
        n = next(counter)
        return pltpu.make_async_remote_copy(src_ref=src, dst_ref=dst, send_sem=ss.at[n], recv_sem=rs.at[n],
                                            device_id=dev, device_id_type=MESH)

    n_tab = tab_sem.shape[0]
    tab_copies = []
    tiles = table.shape[0] - 1
    for i in range(n_tab):
        lo, hi = tiles * i // n_tab, tiles * (i + 1) // n_tab
        tab_copies.append(pltpu.make_async_copy(table_hbm.at[pl.ds(lo, hi - lo)], table.at[pl.ds(lo, hi - lo)],
                                                tab_sem.at[i]))

    barrier = pltpu.get_barrier_semaphore()
    for dev in (sib, up, dn, pair):
        pl.semaphore_signal(barrier, inc=1, device_id=dev, device_id_type=MESH)
    for copy in tab_copies:
        copy.start()
    pl.semaphore_wait(barrier, 4)

    hh = hid // 2

    def wrow(j, c, h=None):
        start = (j * 2 + c) * hid
        if h is None:
            return pl.ds(pl.multiple_of(start, 16), hid)
        return pl.ds(pl.multiple_of(start + h * hh, 16), hh)

    hrow = pl.ds(pl.multiple_of(half * hh, 16), hh)
    w_in = {1: w1_hbm, 2: w2_hbm}
    w_all = {1: w1_all, 2: w2_all}

    wx, wy, wd = {}, {}, {}
    for m in (1, 2):
        wx[1, m] = rcopy(w_in[m].at[hrow], w_all[m].at[wrow(1, core, half)], up)
        wx[3, m] = rcopy(w_in[m].at[hrow], w_all[m].at[wrow(3, core, half)], dn)
    split = hid * 9 // 38 // 16 * 16

    def far(j, part):
        which = half if part in (0, 1) else 1 - half
        start = (j * 2 + core) * hid + which * hh
        if part in (1, 2):
            return pl.ds(pl.multiple_of(start, 16), split)
        return pl.ds(pl.multiple_of(start + split, 16), hh - split)

    for part in (1, 0, 3):
        wx[2, 1, part] = rcopy(w1_all.at[far(1, part)], w1_all.at[far(2, part)], up)
        wx[2, 2, part] = rcopy(w2_all.at[far(3, part)], w2_all.at[far(2, part)], dn)
    for m in (1, 2):
        wy[2, m] = rcopy(w_all[m].at[far(2, 1)], w_all[m].at[far(2, 1)], pair)
        for part in range(4):
            wd[2, m, part] = rcopy(w_all[m].at[far(2, part)], w_all[m].at[far(2, part)], sib)
    for m in (1, 2):
        for j in (1, 3):
            wy[j, m] = rcopy(w_all[m].at[wrow(j, core, half)], w_all[m].at[wrow(j, core, half)], pair)
        wd[0, m] = rcopy(w_in[m], w_all[m].at[wrow(0, core)], sib)
        for j in (1, 3):
            for k, h in ((0, half), (1, 1 - half)):
                wd[j, m, k] = rcopy(w_all[m].at[wrow(j, core, h)], w_all[m].at[wrow(j, core, h)], sib)

    d2d = {}
    for n, j in enumerate((2, 1, 3, 0)):
        d2d[j] = rcopy(for_sib.at[pl.ds((n % 2) * cap, cap)], sib_part.at[pl.ds(j * cap, cap)], sib)
    def of(ref, block, at, size):
        return ref.at[pl.ds(block * cap + at, size)]

    rows = {
        "2ue": rcopy(of(own, 1, base, eh), fwd_up.at[pl.ds(b_lo, eh)], up),
        "2de": rcopy(of(own, 1, base + eh, eh), fwd_dn.at[pl.ds(b_hi, eh)], dn),
        "2ub": rcopy(of(own, 1, 0, b_lo), fwd_up.at[pl.ds(0, b_lo)], up),
        "2db": rcopy(of(own, 1, b_lo, b_hi), fwd_dn.at[pl.ds(0, b_hi)], dn),
        "1b": rcopy(of(own, 0, 0, base), of(got, 1, 0, base), up),
        "1h": rcopy(of(own, 0, base + eh, eh), of(got, 1, base + eh, eh), up),
        "1l": rcopy(of(own, 0, base, eh), of(got, 1, base, eh), up),
        "3b": rcopy(of(own, 2, 0, base), of(got, 3, 0, base), dn),
        "3l": rcopy(of(own, 2, base, eh), of(got, 3, base, eh), dn),
        "3h": rcopy(of(own, 2, base + eh, eh), of(got, 3, base + eh, eh), dn),
        "fu": rcopy(fwd_up.at[pl.ds(0, b_lo)], of(got, 2, 0, b_lo), up),
        "fd": rcopy(fwd_dn.at[pl.ds(0, b_hi)], of(got, 2, b_lo, b_hi), dn),
    }

    for key in ((1, 1), (3, 1), (1, 2), (3, 2)):
        wx[key].start()
    wd[0, 1].start()
    wd[0, 2].start()
    slot_tables(ids_ref, keys, slots_v, over_ref, chip, tp, chips, tiles * SUB, base)
    table[tiles] = jnp.zeros((SUB, width), jnp.bfloat16)
    lanes = slots_v.shape[1]
    fetch = [
        pltpu.make_async_copy(slots_v.at[d], sidx.at[pl.ds(d * lanes, lanes)], loc_sem.at[4 * chips + 2 + d])
        for d in range(2 * chips)
    ]
    for copy in fetch:
        copy.start()
    for copy in fetch:
        copy.wait()
    for copy in tab_copies:
        copy.wait()

    def pick_slots(j, c, dst, at):
        line = (lax.rem(chip + j, chips) * 2 + c) * lanes

        def body(i, carry):
            dst[pl.ds(pl.multiple_of(at + i * 16, 16), 16), :] = pick_16(table, sidx, line + i * 16)
            return carry

        lax.fori_loop(0, cap // 16, body, 0)

    def add_part(j):
        d2d[j].wait_recv()
        ref, at = (got, 0) if j == 0 else (own, (j - 1) * cap)

        def body(i, carry):
            a = pl.ds(pl.multiple_of(at + i * 16, 16), 16)
            ref[a, :] = ref[a, :] + sib_part[pl.ds(pl.multiple_of(j * cap + i * 16, 16), 16), :]
            return carry

        lax.fori_loop(0, cap // 16, body, 0, unroll=3)

    def add_far(at, far_ref, far_at):
        def body(i, carry):
            a = pl.ds(pl.multiple_of(at + i * 16, 16), 16)
            own[a, :] = own[a, :] + far_ref[pl.ds(pl.multiple_of(far_at + i * 16, 16), 16), :]
            return carry

        lax.fori_loop(0, eh // 16, body, 0)

    def pick_sib(n, j):
        pick_slots(j, other, for_sib, (n % 2) * cap)
        d2d[j].start()

    def pick_own(j):
        if j == 0:
            pick_slots(j, core, got, 0)
        else:
            pick_slots(j, core, own, (j - 1) * cap)

    pick_sib(0, 2)
    pick_own(2)
    pick_sib(1, 1)
    add_part(2)
    for key in ("2ue", "2de", "2ub", "2db"):
        rows[key].start()
    pick_own(1)
    d2d[2].wait_send()
    pick_sib(2, 3)
    add_part(1)
    rows["1b"].start()
    rows["1h"].start()
    for j in (1, 3):
        wx[j, 1].wait_recv()
        wy[j, 1].start()
    pick_own(3)
    add_part(3)
    rows["3b"].start()
    rows["3l"].start()
    for j in (3, 1):
        wx[j, 2].wait_recv()
        wy[j, 2].start()
    d2d[1].wait_send()
    pick_sib(3, 0)
    pick_own(0)
    add_part(0)

    slot = {0: 0, 3: 1, 1: 0, 2: 1}
    piece = 2 * hid
    load = {}
    for j in range(chips):
        for m in (1, 2):
            w_at = (slot[j] * 2 + m - 1) * piece
            n = (j * 2 + m - 1) * 2
            if j == 0:
                load[j, m] = [
                    pltpu.make_async_copy(w_in[m], w_buf.at[pl.ds(pl.multiple_of(w_at + core * hid, 16), hid)],
                                          loc_sem.at[n]),
                    pltpu.make_async_copy(w_all[m].at[wrow(0, other)],
                                          w_buf.at[pl.ds(pl.multiple_of(w_at + other * hid, 16), hid)],
                                          loc_sem.at[n + 1]),
                ]
            else:
                load[j, m] = [
                    pltpu.make_async_copy(w_all[m].at[pl.ds(j * piece, piece)], w_buf.at[pl.ds(w_at, piece)],
                                          loc_sem.at[n])
                ]

    def start_load(j):
        for m in (1, 2):
            for copy in load[j, m]:
                copy.start()

    for m in (1, 2):
        wd[0, m].wait_recv()
    start_load(0)
    rows["2ue"].wait_recv()
    add_far(base, fwd_up, b_lo)
    rows["1l"].start()
    rows["2de"].wait_recv()
    add_far(2 * cap + base + eh, fwd_dn, b_hi)
    rows["3h"].start()
    rows["2ub"].wait_recv()
    rows["fu"].start()
    rows["2db"].wait_recv()
    rows["fd"].start()
    for part in (1, 0):
        for m in (1, 2):
            wx[2, m, part].start()
    for j in (1, 3):
        for m in (1, 2):
            wd[j, m, 0].start()

    def crossed(j, m):
        wy[j, m].wait_recv()
        wd[j, m, 1].start()
        if (j, m) == (1, 1) or (j, m) == (3, 2):
            wx[2, m, 3].start()

    crossed(1, 1)
    crossed(3, 1)

    gain = gain_ref[...].astype(jnp.float32)
    lines = tokens // 128
    slot_id = lax.broadcasted_iota(jnp.int32, (128, cap), 1).astype(jnp.float32)

    def place(sources, start, finish):
        def body(i, carry):
            at = pl.ds(pl.multiple_of(i * 512, 512), 512)
            total = None if start else y_ref[at, :]
            def line_of(j):
                line = lax.rem(chip + chips - j, chips) * ids_ref.shape[0] + tp * lines
                return keys[pl.ds(pl.multiple_of(line, SUB), SUB), :].astype(jnp.float32)

            anyone = line_of(0)
            for j in range(1, chips):
                anyone = jnp.maximum(anyone, line_of(j))
            any_t = jnp.transpose(anyone)
            lane = lax.broadcasted_iota(jnp.int32, any_t.shape, 1)

            def column(key_t, r):
                return jnp.sum(jnp.where(lane == 4 * i + r, key_t, 0.0), axis=1, keepdims=True)

            for j in sources:
                size = base if j == 2 else cap
                ids_of = slot_id[:, :size]
                key_t = jnp.transpose(line_of(j))
                hits = []
                for r in range(4):
                    want = jnp.where(ids_of < base, column(key_t, r), column(any_t, r))
                    hits.append(jnp.where(want == ids_of, 1.0, 0.0).astype(jnp.bfloat16))
                part = jnp.dot(jnp.concatenate(hits, axis=0), got[pl.ds(j * cap, size), :],
                               preferred_element_type=jnp.float32)
                total = part if total is None else total + part
            if not finish:
                y_ref[at, :] = total
                return carry
            inv = lax.rsqrt(jnp.mean(total * total, axis=-1, keepdims=True) + RMS_EPS)
            sib_part[at, :] = total.astype(jnp.bfloat16)
            sib_part[pl.ds(pl.multiple_of(tokens + i * 512, 512), 512), :] = (total * inv * gain).astype(jnp.bfloat16)
            return carry

        lax.fori_loop(0, tokens // 512, body, 0)

    place((0,), True, False)
    for key in ("1b", "3b", "1h", "3l", "1l", "3h"):
        rows[key].wait_recv()
    place((1, 3), False, False)
    crossed(3, 2)
    rows["fu"].wait_recv()
    rows["fd"].wait_recv()
    place((2,), False, True)

    block = 512

    def mlp(j, first=False, last=False):
        for m in (1, 2):
            for copy in load[j, m]:
                copy.wait()
        w_at = slot[j] * 2 * piece

        def body(i, carry):
            at = pl.ds(pl.multiple_of(i * block, block), block)
            n = sib_part[pl.ds(pl.multiple_of(tokens + i * block, block), block), :]
            u = lax.dot_general(n, w_buf[pl.ds(w_at, piece), :], (((1,), (1,)), ((), ())),
                                preferred_element_type=jnp.float32)
            y = jnp.dot(gelu(u), w_buf[pl.ds(w_at + piece, piece), :], preferred_element_type=jnp.float32)
            if not first:
                y = y_ref[at, :] + y
            if last:
                sib_part[at, :] = (sib_part[at, :].astype(jnp.float32) + y).astype(jnp.bfloat16)
            else:
                y_ref[at, :] = y
            return carry

        lax.fori_loop(0, tokens // block, body, 0)

    def arrived(j):
        for m in (1, 2):
            for k in range(4 if j == 2 else 2):
                wd[j, m, k].wait_recv()
        start_load(j)

    arrived(3)
    mlp(0, first=True)
    for m in (1, 2):
        wx[2, m, 1].wait_recv()
        wy[2, m].start()
        wd[2, m, 1].start()
    crossed(1, 2)
    mlp(3)
    arrived(1)
    for m in (1, 2):
        wx[2, m, 0].wait_recv()
        wd[2, m, 0].start()
    mlp(1)
    for m in (1, 2):
        wx[2, m, 3].wait_recv()
        wd[2, m, 3].start()
    for m in (1, 2):
        wy[2, m].wait_recv()
        wd[2, m, 2].start()
    arrived(2)
    mlp(2, last=True)
    store = pltpu.make_async_copy(sib_part.at[pl.ds(0, tokens)], out_hbm, loc_sem.at[4 * chips + 1])
    store.start()
    store.wait()

    d2d[3].wait_send()
    d2d[0].wait_send()
    for group in (wx, wy, wd, rows):
        for copy in group.values():
            copy.wait_send()


def copy_kernel(src, dst):
    dst[...] = src[...]


def settle(res):
    rows, width = res.shape
    spec = pl.BlockSpec((rows // 4, width), lambda i: (i, 0))
    return pl.pallas_call(
        copy_kernel,
        out_shape=jax.ShapeDtypeStruct(res.shape, res.dtype),
        grid=(4,),
        in_specs=[spec],
        out_specs=spec,
    )(res)


def solution(mesh):
    ranks = mesh.shape["tp"]
    chips = ranks // 2

    def device_step(token_ids, table, norm_gain, w1, w2):
        shard_rows, width = table.shape
        tokens = token_ids.shape[0] // ranks
        tp = lax.axis_index("tp")
        base, ext = slot_split(tokens)
        cap = base + ext
        low = (base // 2 + 15) // 16 * 16
        hidden = w1.shape[1]
        bf, f32 = jnp.bfloat16, jnp.float32
        dma = pltpu.SemaphoreType.DMA
        anyspec = pl.BlockSpec(memory_space=pl.ANY)
        vmem = pl.BlockSpec(memory_space=pltpu.VMEM)
        lines = token_ids.shape[0] // 128
        lanes = -(-cap // 128) * 128
        out, top, w1_all, w2_all = pl.pallas_call(
            functools.partial(block_kernel, chips),
            out_shape=[
                jax.ShapeDtypeStruct((tokens, width), bf),
                jax.ShapeDtypeStruct((SUB, 128), f32),
                jax.ShapeDtypeStruct((ranks * hidden, width), bf),
                jax.ShapeDtypeStruct((ranks * hidden, width), bf),
            ],
            in_specs=[vmem, anyspec, vmem, anyspec, anyspec],
            out_specs=[anyspec, vmem, anyspec, anyspec],
            scratch_shapes=[
                pltpu.VMEM((shard_rows // SUB + 1, SUB, width), bf),
                pltpu.VMEM((3 * cap, width), bf),
                pltpu.VMEM((4 * cap, width), bf),
                pltpu.VMEM((2 * cap, width), bf),
                pltpu.VMEM((4 * cap, width), bf),
                pltpu.VMEM((low + ext // 2, width), bf),
                pltpu.VMEM((base - low + ext // 2, width), bf),
                pltpu.VMEM((tokens, width), f32),
                pltpu.VMEM((8 * hidden, width), bf),
                pltpu.VMEM((chips * lines, 128), jnp.int32),
                pltpu.VMEM((ranks, lanes), jnp.int32),
                pltpu.SMEM((ranks * lanes,), jnp.int32),
                dma((8,)), dma((4 * chips + 2 + ranks,)),
                dma((N_COPIES,)), dma((N_COPIES,)),
            ],
            compiler_params=pltpu.CompilerParams(
                collective_id=0, has_side_effects=True, vmem_limit_bytes=67043328
            ),
        )(token_ids.reshape(lines, 128), table.reshape(shard_rows // SUB, SUB, width), norm_gain.reshape(1, width), w1.T, w2)
        overflow = top[0, 0] >= cap

        def plain(_):
            local = token_ids - tp * shard_rows
            owned = (local >= 0) & (local < shard_rows)
            found = jnp.take(table, jnp.clip(local, 0, shard_rows - 1), axis=0, mode="clip")
            part = jnp.where(owned[:, None], found, jnp.zeros((), bf)).reshape(ranks, tokens, width)
            x = jnp.sum(lax.all_to_all(part, "tp", 0, 0).astype(f32), axis=0)
            w1s = lax.dynamic_update_slice(w1_all, w1.T, ((tp % 2) * hidden, 0))
            w2s = lax.dynamic_update_slice(w2_all, w2, ((tp % 2) * hidden, 0))
            inv = lax.rsqrt(jnp.mean(x * x, axis=-1, keepdims=True) + RMS_EPS)
            n = (x * inv * norm_gain.astype(f32)).astype(bf)
            u = lax.dot_general(n, w1s, (((1,), (1,)), ((), ())), preferred_element_type=f32)
            y = jnp.dot(gelu(u), w2s, preferred_element_type=f32)
            return (x + y).astype(bf)

        return lax.cond(overflow, plain, settle, out)

    return jax.shard_map(
        device_step,
        mesh=mesh,
        in_specs=(P("dp"), P("tp", None), P(), P(None, "tp"), P("tp", None)),
        out_specs=P(("dp", "tp"), None),
        check_vma=False,
    )
```
